16 devices in a mesh: dp: 2 (over z), col: 2 (over y), fsdp: 4 (over x, core).
Axes of the slice: x: 2, y: 2, z: 2, core: 2. Of those that a mesh axis runs over, the one named last changes fastest.
Arguments:
- x_act: bfloat16 [65536, 768], P(('dp', 'col', 'fsdp'))
- dy_out: bfloat16 [65536, 768], P(('dp', 'col', 'fsdp'))
- w_gate: bfloat16 [768, 2048], P(None, ('col', 'fsdp'))
- w_up: bfloat16 [768, 2048], P(None, ('col', 'fsdp'))
- w_down: bfloat16 [2048, 768], P(('col', 'fsdp'))
- v_gate: bfloat16 [768, 2048], P(None, ('col', 'fsdp'))
- v_up: bfloat16 [768, 2048], P(None, ('col', 'fsdp'))
- v_down: bfloat16 [2048, 768], P(('col', 'fsdp'))
- g_next: float32 [16, 3, 768, 2048], P(('dp', 'col', 'fsdp'))
Outputs:
- output 1: bfloat16 [65536, 768], P(('dp', 'col', 'fsdp'))
- output 2: float32 [3, 768, 2048], P(None, None, ('col', 'fsdp'))
- output 3: float32 [16, 3, 768, 2048], P(('dp', 'col', 'fsdp'))
- output 4: bfloat16 [768, 2048], replicated
- output 5: bfloat16 [768, 2048], replicated
- output 6: bfloat16 [2048, 768], replicated
All inputs are finite; a program needn't handle non-finite values.
Results may differ from the reference program's by a relative error of at most 0.0105826.
Values are sent between devices in bfloat16 or wider.
A program may use at most 1 GiB of HBM per device.

```python
import jax
import jax.numpy as jnp
from jax import lax

D_MODEL = 768
D_FF = 2048
TOKENS_DEV = 4096
N_DEVICES = 16


def draw_normal(key, shape, scaling):
    return jax.random.normal(key, shape, jnp.float32) * scaling


def setup_inputs(seed: int = 0) -> dict:
    keys = jax.random.split(jax.random.key(seed), 9)
    all_rows = N_DEVICES * TOKENS_DEV
    model_scale = D_MODEL ** -0.5
    hidden_scale = D_FF ** -0.5
    return {
        'x_act': draw_normal(keys[0], (all_rows, D_MODEL), 1.0).astype(jnp.bfloat16),
        'dy_out': draw_normal(keys[1], (all_rows, D_MODEL), 1.0).astype(jnp.bfloat16),
        'w_gate': draw_normal(keys[2], (D_MODEL, D_FF), model_scale).astype(jnp.bfloat16),
        'w_up': draw_normal(keys[3], (D_MODEL, D_FF), model_scale).astype(jnp.bfloat16),
        'w_down': draw_normal(keys[4], (D_FF, D_MODEL), hidden_scale).astype(jnp.bfloat16),
        'v_gate': draw_normal(keys[5], (D_MODEL, D_FF), model_scale).astype(jnp.bfloat16),
        'v_up': draw_normal(keys[6], (D_MODEL, D_FF), model_scale).astype(jnp.bfloat16),
        'v_down': draw_normal(keys[7], (D_FF, D_MODEL), hidden_scale).astype(jnp.bfloat16),
        'g_next': draw_normal(keys[8], (N_DEVICES, 3, D_MODEL, D_FF), 1.0),
    }


def reference(x_act, dy_out, w_gate, w_up, w_down, v_gate, v_up, v_down, g_next):
    x_dev = x_act.reshape(N_DEVICES, TOKENS_DEV, D_MODEL)
    dy_dev = dy_out.reshape(N_DEVICES, TOKENS_DEV, D_MODEL)

    def one_device(operands):
        x_loc, dy_loc = operands
        pre_gate = jnp.dot(x_loc, w_gate, preferred_element_type=jnp.float32)
        pre_up = jnp.dot(x_loc, w_up, preferred_element_type=jnp.float32)
        sig_gate = jax.nn.sigmoid(pre_gate)
        act_gate = pre_gate * sig_gate
        hidden = (act_gate * pre_up).astype(jnp.bfloat16)
        d_hidden = jnp.dot(dy_loc, w_down.T, preferred_element_type=jnp.float32)
        d_gate = (d_hidden * pre_up * sig_gate * (1.0 + pre_gate * (1.0 - sig_gate))).astype(jnp.bfloat16)
        d_up = (d_hidden * act_gate).astype(jnp.bfloat16)
        dx_loc = (jnp.dot(d_gate, w_gate.T, preferred_element_type=jnp.float32)
                  + jnp.dot(d_up, w_up.T, preferred_element_type=jnp.float32)).astype(jnp.bfloat16)
        grad_gate = jnp.dot(x_loc.T, d_gate, preferred_element_type=jnp.float32)
        grad_up = jnp.dot(x_loc.T, d_up, preferred_element_type=jnp.float32)
        grad_down_t = jnp.dot(dy_loc.T, hidden, preferred_element_type=jnp.float32)
        return dx_loc, jnp.stack([grad_gate, grad_up, grad_down_t])

    dx_dev, dw_local = lax.map(one_device, (x_dev, dy_dev))
    dx_in = dx_dev.reshape(N_DEVICES * TOKENS_DEV, D_MODEL)
    dw_next = jnp.sum(g_next.astype(jnp.bfloat16).astype(jnp.float32), axis=0)
    return dx_in, dw_next, dw_local, v_gate, v_up, v_down
```

```python
import functools

import jax
import jax.numpy as jnp
from jax import lax
from jax.experimental import pallas as pl
from jax.experimental.pallas import tpu as pltpu
from jax.sharding import PartitionSpec as P

ALL_AXES = ('dp', 'col', 'fsdp')
FSDP_AXES = ('col', 'fsdp')
MESH = pl.DeviceIdType.MESH
bf16, f32 = jnp.bfloat16, jnp.float32

D, FB, TOK = 768, 256, 4096
T = 1024
NT = TOK // T
NA = 6
HALF = D // 2
VMEM_LIMIT = 67043328


def dot(a, b):
    return jnp.dot(a, b, preferred_element_type=f32)


def dot_nt(a, b):
    return lax.dot_general(a, b, (((1,), (1,)), ((), ())), preferred_element_type=f32)


def dot_tn(a, b):
    return lax.dot_general(a, b, (((0,), (0,)), ((), ())), preferred_element_type=f32)


def rows_of(t):
    return pl.ds(pl.multiple_of(t * T, T), T)


def cols_of(b):
    return pl.ds(pl.multiple_of(b * FB, FB), FB)


def phase1(t, w13, w2, x_v, dy_v, ab_s, dh_s):
    rows = rows_of(t)
    ab_s[...] = dot(x_v[rows, :], w13[...])
    dh_s[...] = dot_nt(dy_v[rows, :], w2[...])


def elementwise(ab_s, dh_s, dab_s, h_s):
    a, b, dh = ab_s[:, :FB], ab_s[:, FB:], dh_s[...]
    s = jax.nn.sigmoid(a)
    act = a * s
    h_s[...] = (act * b).astype(bf16)
    dab_s[:, :FB] = (dh * b * s * (1.0 + a * (1.0 - s))).astype(bf16)
    dab_s[:, FB:] = (dh * act).astype(bf16)


def phase2(t, keep_acc, w13, x_v, dy_v, dab_s, h_s, acc_v, dw13, dw2):
    rows = rows_of(t)
    g13 = dot_tn(x_v[rows, :], dab_s[...])
    dw13[...] = jnp.where(t == 0, 0.0, dw13[...]) + g13
    g2 = dot_tn(dy_v[rows, :], h_s[...])
    dw2[...] = jnp.where(t == 0, 0.0, dw2[...]) + g2
    acc = acc_v[rows, :]
    if keep_acc is not None:
        acc = jnp.where(keep_acc, acc, 0.0)
    acc_v[rows, :] = acc + dot_nt(dab_s[...], w13[...])


class Place:
    def __init__(self):
        self.z = lax.axis_index('dp')
        self.y = lax.axis_index('col')
        f = lax.axis_index('fsdp')
        self.x, self.c = f // 2, f % 2
        x, y, z, c = self.x, self.y, self.z, self.c
        self.dev_c = (z, y, x * 2 + 1 - c)
        self.dev_x = (z, y, (1 - x) * 2 + c)
        self.dev_y = (z, 1 - y, x * 2 + c)
        self.dev_z = (1 - z, y, x * 2 + c)
        self.own = self.block(0, 0, c)

    def block(self, flip_x, flip_y, core):
        x = self.x + flip_x * (1 - 2 * self.x)
        y = self.y + flip_y * (1 - 2 * self.y)
        return (y * 2 + x) * 2 + core

    def order(self, j):
        chip = j // 2
        core = self.c + (j % 2) * (1 - 2 * self.c)
        return self.block(chip % 2, chip // 2, core)


def start(copies):
    for c in copies:
        c.start()


def wait(copies):
    for c in copies:
        c.wait()


def weight_copies(src, w13, w2, sem):
    return (pltpu.make_async_copy(src[0], w13.at[:, pl.ds(0, FB)], sem.at[0]),
            pltpu.make_async_copy(src[1], w13.at[:, pl.ds(FB, FB)], sem.at[1]),
            pltpu.make_async_copy(src[2], w2, sem.at[2]))


def main_kernel(x_h, dy_h, w1_h, w3_h, w2_h, v1_h, v3_h, v2_h, g_h,
                lw1, lw3, lw2, lv1, lv3, lv2, acc_h, dw_h, s_h, rz_h,
                x_v, dy_v, w13_v, w2_v, acc_v, dw13_v, dw2_v, ab_s, dh_s, dab_s, h_s,
                g_st, sp, red, rx, ry, r3,
                xs, ws, os, accs, gl, pps, ppr, axs, axr, bys, byr, r3s, r3r, zs, zr, ssem, ags, agr):
    p = Place()
    n_steps = NA * NT
    own_in = ((w1_h, w3_h, w2_h), (v1_h, v3_h, v2_h))
    land = ((lw1, lw3, lw2), (lv1, lv3, lv2))
    is_s = p.c == p.z
    not_s = p.c != p.z
    blk_c, blk_xc, blk_yc, blk_dc = p.order(1), p.order(2), p.order(4), p.order(6)

    def x_copies(t):
        return (pltpu.make_async_copy(x_h.at[rows_of(t)], x_v.at[rows_of(t)], xs.at[0, t]),
                pltpu.make_async_copy(dy_h.at[rows_of(t)], dy_v.at[rows_of(t)], xs.at[1, t]))

    def w_copies(j, slot):
        if isinstance(j, int) and j == 0:
            src = own_in[0]
        else:
            b = p.order(j)
            src = tuple(a.at[b] for a in land[0])
        return weight_copies(src, w13_v.at[slot], w2_v.at[slot], ws.at[slot])

    def out_copies(j, slot):
        return (pltpu.make_async_copy(dw13_v.at[slot, :, pl.ds(0, FB)], dw_h.at[j, 0], os.at[slot, 0]),
                pltpu.make_async_copy(dw13_v.at[slot, :, pl.ds(FB, FB)], dw_h.at[j, 1], os.at[slot, 1]),
                pltpu.make_async_copy(dw2_v.at[slot], dw_h.at[j, 2], os.at[slot, 2]))

    def acc_copy(t):
        return pltpu.make_async_copy(acc_v.at[rows_of(t)], acc_h.at[rows_of(t)], accs.at[t])

    def ag_copy(k, m, own, b, sid, rid, dev):
        src = own_in[k][m] if own else land[k][m].at[b]
        return pltpu.make_async_remote_copy(
            src_ref=src, dst_ref=land[k][m].at[b], send_sem=ags.at[k, sid, m], recv_sem=agr.at[k, rid, m],
            device_id=dev, device_id_type=MESH)

    routes = ((True, p.own, 0, p.dev_c), (True, p.own, 1, p.dev_x), (False, blk_xc, 4, p.dev_c),
              (False, blk_yc, 5, p.dev_c), (False, blk_dc, 6, p.dev_c), (True, p.own, 2, p.dev_y),
              (False, blk_xc, 3, p.dev_y), (False, blk_yc, 2, p.dev_z), (False, blk_dc, 3, p.dev_z))
    arrivals = (blk_c, blk_xc, blk_yc, blk_dc, p.order(3), p.order(5), p.order(7))

    def send(k, sid, parts=(0, 1, 2)):
        own, b, rid, dev = routes[sid]
        for m in parts:
            ag_copy(k, m, own, b, sid, rid, dev).start()

    def wait_sent(k, sid):
        own, b, rid, dev = routes[sid]
        for m in range(3):
            ag_copy(k, m, own, b, sid, rid, dev).wait_send()

    def arrive(k, rid, parts=(0, 1, 2)):
        for m in parts:
            ag_copy(k, m, False, arrivals[rid], 0, rid, p.dev_c).wait_recv()

    def only(cond, fn):
        pl.when(cond)(fn)

    def own_first(k):
        send(k, 0)
        send(k, 1)

    def got_x(k, parts=(0, 1, 2)):
        arrive(k, 1, parts)
        send(k, 2, parts)
        only(is_s, lambda: send(k, 6, parts))

    def got_y(k):
        arrive(k, 2)
        send(k, 3)
        only(is_s, lambda: send(k, 7))

    def got_d(k):
        arrive(k, 3)
        send(k, 4)
        only(is_s, lambda: send(k, 8))

    def g_load(kind, i, u):
        q, m = i // 3, i % 3
        core = p.c if kind else 1 - p.c
        b = p.block(1 - q // 2, 1 - q % 2, core)
        return pltpu.make_async_copy(g_h.at[0, m, :, cols_of(b)], g_st.at[kind, u], gl.at[kind, u])

    def pair_copy(i):
        return pltpu.make_async_remote_copy(
            src_ref=sp.at[i], dst_ref=red.at[i], send_sem=pps.at[i], recv_sem=ppr.at[i],
            device_id=p.dev_c, device_id_type=MESH)

    LO, HI = pl.ds(0, HALF), pl.ds(HALF, HALF)

    def ax_copy(q, m):
        return pltpu.make_async_remote_copy(
            src_ref=red.at[q * 3 + m, LO], dst_ref=rx.at[q, m], send_sem=axs.at[q, m], recv_sem=axr.at[q, m],
            device_id=p.dev_x, device_id_type=MESH)

    def by_copy(h, m):
        return pltpu.make_async_remote_copy(
            src_ref=red.at[h * 6 + m, HI], dst_ref=ry.at[h, m], send_sem=bys.at[h, m], recv_sem=byr.at[h, m],
            device_id=p.dev_y, device_id_type=MESH)

    def r3_copy(way):
        src = red.at[pl.ds(6, 3), LO] if way == 0 else red.at[pl.ds(3, 3), HI]
        return pltpu.make_async_remote_copy(
            src_ref=src, dst_ref=r3.at[way], send_sem=r3s.at[way], recv_sem=r3r.at[way],
            device_id=p.dev_y if way == 0 else p.dev_x, device_id_type=MESH)

    def z_copy(way):
        rows = LO if way == 0 else HI
        return pltpu.make_async_remote_copy(
            src_ref=red.at[pl.ds(9, 3), rows], dst_ref=rz_h.at[:, rows], send_sem=zs.at[way], recv_sem=zr.at[way],
            device_id=p.dev_z, device_id_type=MESH)

    def s_copy(way):
        rows = LO if way == 0 else HI
        return pltpu.make_async_copy(red.at[pl.ds(9, 3), rows], s_h.at[:, rows], ssem.at[way])

    def add_into(q, rows, got):
        for m in range(3):
            red[q * 3 + m, rows, :] = (red[q * 3 + m, rows, :].astype(f32) + got[m].astype(f32)).astype(bf16)

    def g_part(n):
        @pl.when((n >= 1) & (n <= 6))
        def _():
            for u in range(2):
                pair_copy(2 * (n - 1) + u).start()

        @pl.when((n >= 3) & (n <= 8))
        def _():
            for u in range(2):
                i = 2 * (n - 3) + u
                q, m = i // 3, i % 3

                @pl.when(q < 2)
                def _():
                    ax_copy(q, m).start()

                @pl.when((q == 0) | (q == 2))
                def _():
                    by_copy(q // 2, m).start()

        @pl.when(n <= 5)
        def _():
            for u in range(2):
                i = 2 * n + u
                g_load(0, i, u).wait()
                sp[i] = g_st[0, u].astype(bf16)

                @pl.when(n < 5)
                def _():
                    g_load(0, i + 2, u).start()

        @pl.when((n >= 2) & (n <= 7))
        def _():
            for u in range(2):
                i = 2 * (n - 2) + u
                g_load(1, i, u).wait()
                pair_copy(i).wait_recv()
                red[i] = (red[i].astype(f32) + g_st[1, u].astype(bf16).astype(f32)).astype(bf16)

                @pl.when(n < 7)
                def _():
                    g_load(1, i + 2, u).start()

    def add_rx0():
        for m in range(3):
            ax_copy(0, m).wait_recv()
        add_into(2, LO, rx.at[0])

    def add_ry0():
        for m in range(3):
            by_copy(0, m).wait_recv()
        add_into(1, HI, ry.at[0])

    def add_rx1():
        for m in range(3):
            ax_copy(1, m).wait_recv()
        add_into(3, LO, rx.at[1])

    def add_ry1():
        for m in range(3):
            by_copy(1, m).wait_recv()
        add_into(3, HI, ry.at[1])

    def add_r3(way):
        r3_copy(way).wait_recv()
        add_into(3, LO if way == 0 else HI, r3.at[way])

    def send_z(way):
        z_copy(way).start()
        s_copy(way).start()

    def next_weights(j, rid=None):
        if rid is not None:
            arrive(0, rid)
        start(w_copies(j, j % 2))

    events = {
        2: [lambda: next_weights(1, 0)],
        4: [lambda: only(is_s, lambda: got_y(0))],
        6: [lambda: got_x(0), lambda: next_weights(2)],
        8: [add_ry0],
        9: [lambda: r3_copy(1).start(), lambda: only(not_s, lambda: got_y(0))],
        10: [add_rx0, lambda: next_weights(3, 4), lambda: own_first(1)],
        11: [lambda: r3_copy(0).start(), add_ry1],
        12: [lambda: only(is_s, lambda: send(1, 5))],
        13: [add_rx1, lambda: only(is_s, lambda: got_d(0))],
        14: [lambda: next_weights(4)],
        16: [lambda: add_r3(1), lambda: add_r3(0)],
        17: [lambda: send_z(0), lambda: send_z(1), lambda: only(not_s, lambda: got_d(0))],
        18: [lambda: next_weights(5, 5), lambda: got_x(1, (0,))],
        20: [lambda: got_x(1, (1,)), lambda: only(is_s, lambda: got_y(1))],
        22: [lambda: got_x(1, (2,))],
    }

    start(w_copies(0, 0))
    start(x_copies(0))
    for kind in range(2):
        for u in range(2):
            g_load(kind, u, u).start()
    for t in range(1, NT):
        start(x_copies(t))
    barrier = pltpu.get_barrier_semaphore()
    for dev in (p.dev_c, p.dev_x, p.dev_y, p.dev_z):
        pl.semaphore_signal(barrier, inc=1, device_id=dev, device_id_type=MESH)
    pl.semaphore_wait(barrier, 4)
    own_first(0)
    only(is_s, lambda: send(0, 5))
    wait(w_copies(0, 0))
    wait(x_copies(0))
    phase1(0, w13_v.at[0], w2_v.at[0], x_v, dy_v, ab_s, dh_s)

    def step(n, carry):
        j, t = n // NT, n % NT
        ahead = jnp.minimum(n + 1, n_steps - 1)
        j1, t1 = ahead // NT, ahead % NT
        slot, slot1 = j % 2, j1 % 2

        g_part(n)
        for at, fns in events.items():
            def run(fns=fns):
                for fn in fns:
                    fn()
            pl.when(n == at)(run)

        @pl.when((t == 0) & (j >= 2))
        def _():
            wait(out_copies(j - 2, slot))

        @pl.when((t == NT - 1) & (j + 1 < NA))
        def _():
            wait(w_copies(j + 1, 1 - slot))

        @pl.when(n + 1 < NT)
        def _():
            wait(x_copies(t1))

        elementwise(ab_s, dh_s, dab_s, h_s)
        phase1(t1, w13_v.at[slot1], w2_v.at[slot1], x_v, dy_v, ab_s, dh_s)
        phase2(t, j > 0, w13_v.at[slot], x_v, dy_v, dab_s, h_s, acc_v, dw13_v.at[slot], dw2_v.at[slot])

        @pl.when(t == NT - 1)
        def _():
            start(out_copies(j, slot))

        @pl.when(j == NA - 1)
        def _():
            acc_copy(t).start()

        return carry

    lax.fori_loop(0, n_steps, step, 0)

    only(not_s, lambda: got_y(1))
    got_d(1)
    arrive(0, 6)
    arrive(1, 0)
    for rid in (4, 5, 6):
        arrive(1, rid)
    for way in range(2):
        z_copy(way).wait()
        s_copy(way).wait()
        r3_copy(way).wait_send()
    for i in range(12):
        pair_copy(i).wait_send()
    for q in range(2):
        for m in range(3):
            ax_copy(q, m).wait_send()
            by_copy(q, m).wait_send()
    for k in range(2):
        for sid in range(5):
            wait_sent(k, sid)

    def sent_by_s():
        for k in range(2):
            for sid in range(5, 9):
                wait_sent(k, sid)
    only(is_s, sent_by_s)
    for j in (NA - 2, NA - 1):
        wait(out_copies(j, j % 2))
    for t in range(NT):
        acc_copy(t).wait()


def last_kernel(x_h, dy_h, lw1, lw3, lw2, lv1, lv3, lv2, v1_h, v3_h, v2_h, acc_h, dwa_h, s_h, rz_h,
                dx_h, gn_h, dw_h, o1_h, o3_h, o2_h,
                x_v, dy_v, w13_v, w2_v, acc_v, dw13_v, dw2_v, ab_s, dh_s, dab_s, h_s,
                big, col, row, s_v, rz_v, gn_v,
                xs, ws, os, accs, dxs, ins, outs, sz, gs):
    p = Place()
    nb = 8 - NA
    n_steps = nb * NT

    def x_copies(t):
        return (pltpu.make_async_copy(x_h.at[rows_of(t)], x_v.at[rows_of(t)], xs.at[0, t]),
                pltpu.make_async_copy(dy_h.at[rows_of(t)], dy_v.at[rows_of(t)], xs.at[1, t]))

    def acc_copy(t):
        return pltpu.make_async_copy(acc_h.at[rows_of(t)], acc_v.at[rows_of(t)], accs.at[t])

    def dx_copy(t):
        return pltpu.make_async_copy(dy_v.at[rows_of(t)], dx_h.at[rows_of(t)], dxs.at[t])

    def w_copies(j, slot):
        b = p.order(NA + j)
        return weight_copies(tuple(a.at[b] for a in (lw1, lw3, lw2)), w13_v.at[slot], w2_v.at[slot], ws.at[slot])

    def out_copies(j, slot):
        cols = cols_of(p.order(NA + j))
        return (pltpu.make_async_copy(dw13_v.at[slot, :, pl.ds(0, FB)], dw_h.at[0, :, cols], os.at[slot, 0]),
                pltpu.make_async_copy(dw13_v.at[slot, :, pl.ds(FB, FB)], dw_h.at[1, :, cols], os.at[slot, 1]),
                pltpu.make_async_copy(dw2_v.at[slot], dw_h.at[2, :, cols], os.at[slot, 2]))

    moves = []
    for j in range(NA):
        cols = cols_of(p.order(j))
        for m in range(3):
            moves.append(('big', dwa_h.at[j, m], dw_h.at[m, :, cols]))
    vmoves = []
    for j in range(8):
        b = p.order(j)
        for m, (own, got, out) in enumerate(((v1_h, lv1, o1_h), (v3_h, lv3, o3_h), (v2_h, lv2, o2_h))):
            src = own if j == 0 else got.at[b]
            if m < 2:
                vmoves.append(('col', src, out.at[:, cols_of(b)]))
            else:
                vmoves.append(('row', src, out.at[pl.ds(pl.multiple_of(b * FB, FB), FB)]))
    groups = n_steps - 2
    sets = [moves[g::groups] + vmoves[g::groups] for g in range(groups)]

    def staged(g, way):
        copies, used, half = [], {'big': 0, 'col': 0, 'row': 0}, g % 2
        for k, (kind, src, dst) in enumerate(sets[g]):
            buf = {'big': big, 'col': col, 'row': row}[kind].at[half, used[kind]]
            used[kind] += 1
            if way == 0:
                copies.append(pltpu.make_async_copy(src, buf, ins.at[half, k]))
            else:
                copies.append(pltpu.make_async_copy(buf, dst, outs.at[half, k]))
        return copies

    def sz_copies():
        return (pltpu.make_async_copy(s_h, s_v, sz.at[0]), pltpu.make_async_copy(rz_h, rz_v, sz.at[1]))

    def gn_copy():
        return pltpu.make_async_copy(gn_v, gn_h, gs.at[0])

    start(w_copies(0, 0))
    start(x_copies(0))
    start(x_copies(1))
    acc_copy(0).start()
    for t in range(2, NT):
        start(x_copies(t))
        acc_copy(t - 1).start()
    acc_copy(NT - 1).start()
    for j in range(1, nb):
        start(w_copies(j, j))
    start(sz_copies())
    wait(w_copies(0, 0))
    wait(x_copies(0))
    phase1(0, w13_v.at[0], w2_v.at[0], x_v, dy_v, ab_s, dh_s)

    def dw_next():
        wait(sz_copies())
        for m in range(3):
            gn_v[m] = s_v[m].astype(f32) + rz_v[m].astype(f32)
        gn_copy().start()

    def pass_step(k):
        if 1 <= k <= groups:
            wait(staged(k - 1, 0))
            start(staged(k - 1, 1))
        if k < groups:
            if k >= 2:
                wait(staged(k - 2, 1))
            start(staged(k, 0))

    def step(n, carry):
        j, t = n // NT, n % NT
        ahead = jnp.minimum(n + 1, n_steps - 1)
        j1, t1 = ahead // NT, ahead % NT
        slot, slot1 = j % 2, j1 % 2

        @pl.when(n + 1 < NT)
        def _():
            wait(x_copies(t1))

        @pl.when(n < NT)
        def _():
            acc_copy(t).wait()

        @pl.when((t == NT - 1) & (j + 1 < nb))
        def _():
            wait(w_copies(j + 1, 1 - slot))

        for k in range(n_steps):
            pl.when(n == k)(functools.partial(pass_step, k))
        pl.when(n == 3)(dw_next)

        elementwise(ab_s, dh_s, dab_s, h_s)
        phase1(t1, w13_v.at[slot1], w2_v.at[slot1], x_v, dy_v, ab_s, dh_s)
        phase2(t, None, w13_v.at[slot], x_v, dy_v, dab_s, h_s, acc_v, dw13_v.at[slot], dw2_v.at[slot])

        @pl.when(t == NT - 1)
        def _():
            start(out_copies(j, slot))

        @pl.when(j == nb - 1)
        def _():
            dy_v[rows_of(t), :] = acc_v[rows_of(t), :].astype(bf16)
            dx_copy(t).start()

        return carry

    lax.fori_loop(0, n_steps, step, 0)
    for t in range(NT):
        dx_copy(t).wait()
    for g in (groups - 2, groups - 1):
        wait(staged(g, 1))
    for j in range(nb):
        wait(out_copies(j, j))
    gn_copy().wait()


def compute_scratch():
    return [pltpu.VMEM((TOK, D), bf16), pltpu.VMEM((TOK, D), bf16),
            pltpu.VMEM((2, D, 2 * FB), bf16), pltpu.VMEM((2, FB, D), bf16),
            pltpu.VMEM((TOK, D), f32), pltpu.VMEM((2, D, 2 * FB), f32), pltpu.VMEM((2, D, FB), f32),
            pltpu.VMEM((T, 2 * FB), f32), pltpu.VMEM((T, FB), f32),
            pltpu.VMEM((T, 2 * FB), bf16), pltpu.VMEM((T, FB), bf16)]


def solution(mesh):
    anys = pl.BlockSpec(memory_space=pl.ANY)
    dma = pltpu.SemaphoreType.DMA
    sds = jax.ShapeDtypeStruct

    def device_step(x_loc, dy_loc, w_gate, w_up, w_down, v_gate, v_up, v_down, g_next):
        land = [sds((8, D, FB), bf16), sds((8, D, FB), bf16), sds((8, FB, D), bf16)]
        *gathered, acc, dw_part, g_sum, g_other = pl.pallas_call(
            main_kernel,
            out_shape=land + land + [sds((TOK, D), f32), sds((NA, 3, D, FB), f32),
                                     sds((3, D, FB), bf16), sds((3, D, FB), bf16)],
            in_specs=[anys] * 9, out_specs=[anys] * 10,
            scratch_shapes=compute_scratch() + [
                pltpu.VMEM((2, 2, D, FB), f32), pltpu.VMEM((12, D, FB), bf16), pltpu.VMEM((12, D, FB), bf16),
                pltpu.VMEM((2, 3, HALF, FB), bf16), pltpu.VMEM((2, 3, HALF, FB), bf16),
                pltpu.VMEM((2, 3, HALF, FB), bf16),
                dma((2, NT)), dma((2, 3)), dma((2, 3)), dma((NT,)), dma((2, 2)), dma((12,)), dma((12,)),
                dma((2, 3)), dma((2, 3)), dma((2, 3)), dma((2, 3)), dma((2,)), dma((2,)), dma((2,)), dma((2,)),
                dma((2,)), dma((2, 9, 3)), dma((2, 7, 3))],
            compiler_params=pltpu.CompilerParams(
                collective_id=0, has_side_effects=True, vmem_limit_bytes=VMEM_LIMIT),
            name='main_part',
        )(x_loc, dy_loc, w_gate, w_up, w_down, v_gate, v_up, v_down, g_next)
        dx, grad_next, grad_local, vg, vu, vd = pl.pallas_call(
            last_kernel,
            out_shape=[sds((TOK, D), bf16), sds((3, D, FB), f32), sds((3, D, 8 * FB), f32),
                       sds((D, 8 * FB), bf16), sds((D, 8 * FB), bf16), sds((8 * FB, D), bf16)],
            in_specs=[anys] * 15, out_specs=[anys] * 6,
            scratch_shapes=compute_scratch() + [
                pltpu.VMEM((2, 3, D, FB), f32), pltpu.VMEM((2, 4, D, FB), bf16), pltpu.VMEM((2, 4, FB, D), bf16),
                pltpu.VMEM((3, D, FB), bf16), pltpu.VMEM((3, D, FB), bf16), pltpu.VMEM((3, D, FB), f32),
                dma((2, NT)), dma((2, 3)), dma((2, 3)), dma((NT,)), dma((NT,)), dma((2, 8)), dma((2, 8)),
                dma((2,)), dma((1,))],
            compiler_params=pltpu.CompilerParams(vmem_limit_bytes=VMEM_LIMIT),
            name='last_part',
        )(x_loc, dy_loc, *gathered, v_gate, v_up, v_down, acc, dw_part, g_sum, g_other)
        return dx, grad_next, grad_local[None], vg, vu, vd

    row_spec = P(ALL_AXES, None)
    col_shard = P(None, FSDP_AXES)
    row_shard = P(FSDP_AXES, None)
    dev_spec = P(ALL_AXES, None, None, None)
    return jax.shard_map(
        device_step, mesh=mesh,
        in_specs=(row_spec, row_spec, col_shard, col_shard, row_shard, col_shard, col_shard, row_shard, dev_spec),
        out_specs=(row_spec, P(None, None, FSDP_AXES), dev_spec, P(), P(), P()),
        check_vma=False)
```

```python
import functools

import jax
import jax.numpy as jnp
from jax import lax
from jax.experimental import pallas as pl
from jax.experimental.pallas import tpu as pltpu
from jax.sharding import PartitionSpec as P

ALL_AXES = ('dp', 'col', 'fsdp')
FSDP_AXES = ('col', 'fsdp')
MESH = pl.DeviceIdType.MESH
bf16, f32 = jnp.bfloat16, jnp.float32

D, FB, TOK = 768, 256, 4096
T = 1024
NT = TOK // T
NA = 7
Y_FIRST = False
PC = 2
NEXT_AT = 2
V_AT, V_LAG = (0,1,1), 2
DW_GROUPS = 3
SCHEDULE = (
    ('WoX1', 'WoX0', 'WoC', 'VoX10', 'VoY0', 'VoY2'),
    ('WoY',),
    (),
    ('VoC', 'VoX00'),
    (),
    (),
    ('Wgy1', 'Wgx', 'WgxY'),
    (),
    ('VoX11', 'Vgy10'),
    ('Vgy12',),
    ('VoY1',),
    ('Vgx0',),
    ('Wgy0',),
    ('Vgy11',),
    ('ay0', 'VoX01'),
    ('r3s1', 'Wgd1', 'VgxY0'),
    ('ax0', 'VoX12'),
    ('Vgd10', 'Vgx1', 'VgxY1', 'Vgy01'),
    ('r3s0',),
    ('Vgd11',),
    ('ay1', 'ra1', 'VoX02'),
    ('zs1', 'Vgd01'),
    ('Vgy00', 'Vgx2', 'VgxY2', 'Vgy02'),
    ('ax1', 'ra0', 'Vgd12'),
    ('zs0',),
    ('Vgd00',),
    ('Wgd0', 'Vgd02'),
    (),
    (),
)
HALF = D // 2
VMEM_LIMIT = 67043328


def dot(a, b):
    return jnp.dot(a, b, preferred_element_type=f32)


def dot_nt(a, b):
    return lax.dot_general(a, b, (((1,), (1,)), ((), ())), preferred_element_type=f32)


def dot_tn(a, b):
    return lax.dot_general(a, b, (((0,), (0,)), ((), ())), preferred_element_type=f32)


def rows_of(t):
    return pl.ds(pl.multiple_of(t * T, T), T)


def cols_of(b):
    return pl.ds(pl.multiple_of(b * FB, FB), FB)


def phase1(t, w13, w2, x_v, dy_v, ab_s, dh_s):
    rows = rows_of(t)
    ab_s[...] = dot(x_v[rows, :], w13[...])
    dh_s[...] = dot_nt(dy_v[rows, :], w2[...])


def elementwise(ab_s, dh_s, dab_s, h_s):
    a, b, dh = ab_s[:, :FB], ab_s[:, FB:], dh_s[...]
    s = jax.nn.sigmoid(a)
    act = a * s
    h_s[...] = (act * b).astype(bf16)
    dab_s[:, :FB] = (dh * b * s * (1.0 + a * (1.0 - s))).astype(bf16)
    dab_s[:, FB:] = (dh * act).astype(bf16)


def fresh(t, ref):
    return ref[...] if isinstance(t, int) else jnp.where(t == 0, 0.0, ref[...])


def phase2(t, keep_acc, w13, x_v, dy_v, dab_s, h_s, acc_v, dw13, dw2):
    rows = rows_of(t)
    g13 = dot_tn(x_v[rows, :], dab_s[...])
    dw13[...] = fresh(t, dw13) + g13
    g2 = dot_tn(dy_v[rows, :], h_s[...])
    dw2[...] = fresh(t, dw2) + g2
    acc = acc_v[rows, :]
    if keep_acc is not None:
        acc = acc if keep_acc is True else jnp.where(keep_acc, acc, 0.0)
    acc_v[rows, :] = acc + dot_nt(dab_s[...], w13[...])


class Place:
    def __init__(self):
        self.z = lax.axis_index('dp')
        self.y = lax.axis_index('col')
        f = lax.axis_index('fsdp')
        self.x, self.c = f // 2, f % 2
        x, y, z, c = self.x, self.y, self.z, self.c
        self.dev_c = (z, y, x * 2 + 1 - c)
        self.dev_x = (z, y, (1 - x) * 2 + c)
        self.dev_y = (z, 1 - y, x * 2 + c)
        self.dev_z = (1 - z, y, x * 2 + c)
        self.own = self.block(0, 0, c)

    def block(self, flip_x, flip_y, core):
        x = self.x + flip_x * (1 - 2 * self.x)
        y = self.y + flip_y * (1 - 2 * self.y)
        return (y * 2 + x) * 2 + core

    def order(self, j):
        chip = j // 2
        first = self.c + (chip // 3) * (self.z - self.c)
        core = first + (j % 2) * (1 - 2 * first)
        return self.block(chip // 2, chip % 2, core) if Y_FIRST else self.block(chip % 2, chip // 2, core)


def when(cond, fn):
    if isinstance(cond, bool):
        if cond:
            fn()
    else:
        pl.when(cond)(fn)


def start(copies):
    for c in copies:
        c.start()


def wait(copies):
    for c in copies:
        c.wait()


def weight_copies(src, w13, w2, sem):
    return (pltpu.make_async_copy(src[0], w13.at[:, pl.ds(0, FB)], sem.at[0]),
            pltpu.make_async_copy(src[1], w13.at[:, pl.ds(FB, FB)], sem.at[1]),
            pltpu.make_async_copy(src[2], w2, sem.at[2]))


def main_kernel(x_h, dy_h, w1_h, w3_h, w2_h, v1_h, v3_h, v2_h, g_h,
                lw1, lw3, lw2, lv1, lv3, lv2, acc_h, dw_h, s_h, rz_h,
                x_v, dy_v, w13_v, w2_v, acc_v, dw13_v, dw2_v, ab_s, dh_s, dab_s, h_s,
                g_st, sp, red, rx, ry, r3,
                xs, ws, os, accs, gl, pps, ppr, axs, axr, bys, byr, r3s, r3r, zs, zr, ssem, ags, agr):
    p = Place()
    n_steps = NA * NT
    own_in = ((w1_h, w3_h, w2_h), (v1_h, v3_h, v2_h))
    land = ((lw1, lw3, lw2), (lv1, lv3, lv2))
    role = (p.c == p.z, p.c != p.z)
    blk_c, blk_xc, blk_yc, blk_dc = (p.block(0, 0, 1 - p.c), p.block(1, 0, p.c), p.block(0, 1, p.c), p.block(1, 1, p.c))
    def x_copies(t):
        return (pltpu.make_async_copy(x_h.at[rows_of(t)], x_v.at[rows_of(t)], xs.at[0, t]),
                pltpu.make_async_copy(dy_h.at[rows_of(t)], dy_v.at[rows_of(t)], xs.at[1, t]))

    def w_copies(j, slot):
        if isinstance(j, int) and j == 0:
            src = own_in[0]
        else:
            b = p.order(j)
            src = tuple(a.at[b] for a in land[0])
        return weight_copies(src, w13_v.at[slot], w2_v.at[slot], ws.at[slot])

    def out_copies(j, slot):
        return (pltpu.make_async_copy(dw13_v.at[slot, :, pl.ds(0, FB)], dw_h.at[j, 0], os.at[slot, 0]),
                pltpu.make_async_copy(dw13_v.at[slot, :, pl.ds(FB, FB)], dw_h.at[j, 1], os.at[slot, 1]),
                pltpu.make_async_copy(dw2_v.at[slot], dw_h.at[j, 2], os.at[slot, 2]))

    def acc_copy(t):
        return pltpu.make_async_copy(acc_v.at[rows_of(t)], acc_h.at[rows_of(t)], accs.at[t])

    def ag_copy(k, m, own, b, sid, rid, dev):
        src = own_in[k][m] if own else land[k][m].at[b]
        return pltpu.make_async_remote_copy(
            src_ref=src, dst_ref=land[k][m].at[b], send_sem=ags.at[k, sid, m], recv_sem=agr.at[k, rid, m],
            device_id=dev, device_id_type=MESH)

    routes = ((True, p.own, 0, p.dev_c), (True, p.own, 1, p.dev_x), (False, blk_xc, 4, p.dev_c),
              (False, blk_yc, 5, p.dev_c), (False, blk_dc, 6, p.dev_c), (True, p.own, 2, p.dev_y),
              (False, blk_xc, 3, p.dev_y), (False, blk_yc, 2, p.dev_z), (False, blk_dc, 3, p.dev_z))
    arrivals = (blk_c, blk_xc, blk_yc, blk_dc, p.block(1, 0, 1 - p.c), p.block(0, 1, 1 - p.c), p.block(1, 1, 1 - p.c))

    def send(k, sid, parts=(0, 1, 2)):
        own, b, rid, dev = routes[sid]
        for m in parts:
            ag_copy(k, m, own, b, sid, rid, dev).start()

    def wait_sent(k, sid):
        own, b, rid, dev = routes[sid]
        for m in range(3):
            ag_copy(k, m, own, b, sid, rid, dev).wait_send()

    def arrive(k, rid, parts=(0, 1, 2)):
        for m in parts:
            ag_copy(k, m, False, arrivals[rid], 0, rid, p.dev_c).wait_recv()

    def by_role(k, r, fn):
        pl.when(role[k] if r else role[1 - k])(fn)

    def own_x(k, r, parts):
        by_role(k, r, lambda: send(k, 1, parts))

    def own_y(k, parts):
        by_role(k, True, lambda: send(k, 5, parts))

    def got_x(k, parts):
        arrive(k, 1, parts)
        send(k, 2, parts)

    def x_to_y(k, parts):
        by_role(k, True, lambda: send(k, 6, parts))

    def got_y(k, r, parts):
        def body():
            arrive(k, 2, parts)
            send(k, 3, parts)
            if r:
                send(k, 7, parts)
        by_role(k, r, body)

    def got_d(k, r, parts):
        def body():
            arrive(k, 3, parts)
            send(k, 4, parts)
            if r:
                send(k, 8, parts)
        by_role(k, r, body)

    def g_load(kind, i, u):
        q, m = i // 3, i % 3
        core = p.c if kind else 1 - p.c
        b = p.block(1 - q // 2, 1 - q % 2, core)
        return pltpu.make_async_copy(g_h.at[0, m, :, cols_of(b)], g_st.at[kind, u], gl.at[kind, u])

    def pair_copy(i):
        return pltpu.make_async_remote_copy(
            src_ref=sp.at[i], dst_ref=red.at[i], send_sem=pps.at[i], recv_sem=ppr.at[i],
            device_id=p.dev_c, device_id_type=MESH)

    LO, HI = pl.ds(0, HALF), pl.ds(HALF, HALF)

    def ax_copy(q, m):
        return pltpu.make_async_remote_copy(
            src_ref=red.at[q * 3 + m, LO], dst_ref=rx.at[q, m], send_sem=axs.at[q, m], recv_sem=axr.at[q, m],
            device_id=p.dev_x, device_id_type=MESH)

    def by_copy(h, m):
        return pltpu.make_async_remote_copy(
            src_ref=red.at[h * 6 + m, HI], dst_ref=ry.at[h, m], send_sem=bys.at[h, m], recv_sem=byr.at[h, m],
            device_id=p.dev_y, device_id_type=MESH)

    def r3_copy(way):
        src = red.at[pl.ds(6, 3), LO] if way == 0 else red.at[pl.ds(3, 3), HI]
        return pltpu.make_async_remote_copy(
            src_ref=src, dst_ref=r3.at[way], send_sem=r3s.at[way], recv_sem=r3r.at[way],
            device_id=p.dev_y if way == 0 else p.dev_x, device_id_type=MESH)

    def z_copy(way):
        rows = LO if way == 0 else HI
        return pltpu.make_async_remote_copy(
            src_ref=red.at[pl.ds(9, 3), rows], dst_ref=rz_h.at[:, rows], send_sem=zs.at[way], recv_sem=zr.at[way],
            device_id=p.dev_z, device_id_type=MESH)

    def s_copy(way):
        rows = LO if way == 0 else HI
        return pltpu.make_async_copy(red.at[pl.ds(9, 3), rows], s_h.at[:, rows], ssem.at[way])

    def add_into(q, rows, got):
        for m in range(3):
            red[q * 3 + m, rows, :] = (red[q * 3 + m, rows, :].astype(f32) + got[m].astype(f32)).astype(bf16)

    g_steps = 12 // PC

    def g_part(n):
        def pair_sends():
            for u in range(PC):
                pair_copy(PC * (n - 1) + u).start()
        when((n >= 1) & (n <= g_steps), pair_sends)

        def first_sends():
            for u in range(PC):
                i = PC * (n - 3) + u
                q, m = i // 3, i % 3

                @pl.when(q < 2)
                def _():
                    ax_copy(q, m).start()

                @pl.when((q == 0) | (q == 2))
                def _():
                    by_copy(q // 2, m).start()
        when((n >= 3) & (n < 3 + g_steps), first_sends)

        def casts():
            for u in range(PC):
                i = PC * n + u
                g_load(0, i, u).wait()
                sp[i] = g_st[0, u].astype(bf16)

                @pl.when(n < g_steps - 1)
                def _():
                    g_load(0, i + PC, u).start()
        when(n < g_steps, casts)

        def pair_adds():
            for u in range(PC):
                i = PC * (n - 2) + u
                g_load(1, i, u).wait()
                pair_copy(i).wait_recv()
                red[i] = (red[i].astype(f32) + g_st[1, u].astype(bf16).astype(f32)).astype(bf16)

                @pl.when(n < g_steps + 1)
                def _():
                    g_load(1, i + PC, u).start()
        when((n >= 2) & (n < 2 + g_steps), pair_adds)

    def add_rx0():
        for m in range(3):
            ax_copy(0, m).wait_recv()
        add_into(2, LO, rx.at[0])

    def add_ry0():
        for m in range(3):
            by_copy(0, m).wait_recv()
        add_into(1, HI, ry.at[0])

    def add_rx1():
        for m in range(3):
            ax_copy(1, m).wait_recv()
        add_into(3, LO, rx.at[1])

    def add_ry1():
        for m in range(3):
            by_copy(1, m).wait_recv()
        add_into(3, HI, ry.at[1])

    def add_r3(way):
        r3_copy(way).wait_recv()
        add_into(3, LO if way == 0 else HI, r3.at[way])

    def send_z(way):
        z_copy(way).start()
        s_copy(way).start()

    def next_weights(j):
        if j % 2:
            arrive(0, {1: 0, 3: 5 if Y_FIRST else 4, 5: 4 if Y_FIRST else 5}[j])
        if j == 6:
            by_role(0, False, lambda: arrive(0, 6))
        start(w_copies(j, j % 2))

    W3 = (0, 1, 2)
    actions = {
        'r3s1': lambda: r3_copy(1).start(), 'r3s0': lambda: r3_copy(0).start(),
        'zs0': lambda: send_z(0), 'zs1': lambda: send_z(1),
        'WoX1': lambda: own_x(0, True, W3), 'WoX0': lambda: own_x(0, False, W3), 'WoC': lambda: send(0, 0),
        'WoY': lambda: own_y(0, W3), 'Wgy1': lambda: got_y(0, True, W3), 'Wgx': lambda: got_x(0, W3),
        'WgxY': lambda: x_to_y(0, W3), 'Wgy0': lambda: got_y(0, False, W3),
        'Wgd1': lambda: got_d(0, True, W3), 'Wgd0': lambda: got_d(0, False, W3),
        'ay0': add_ry0, 'ax0': add_rx0, 'ax1': add_rx1, 'ay1': add_ry1,
        'ra1': lambda: add_r3(1), 'ra0': lambda: add_r3(0), 'VoC': lambda: send(1, 0)}
    for m in range(3):
        actions[f'VoX1{m}'] = functools.partial(own_x, 1, True, (m,))
        actions[f'VoX0{m}'] = functools.partial(own_x, 1, False, (m,))
        actions[f'VoY{m}'] = functools.partial(own_y, 1, (m,))
    for m in range(3):
        actions[f'Vgx{m}'] = functools.partial(got_x, 1, (m,))
        actions[f'VgxY{m}'] = functools.partial(x_to_y, 1, (m,))
        actions[f'Vgy1{m}'] = functools.partial(got_y, 1, True, (m,))
        actions[f'Vgy0{m}'] = functools.partial(got_y, 1, False, (m,))
        actions[f'Vgd1{m}'] = functools.partial(got_d, 1, True, (m,))
        actions[f'Vgd0{m}'] = functools.partial(got_d, 1, False, (m,))
    assert len(SCHEDULE) == n_steps + 1
    events = {at: [actions[name] for name in names] for at, names in enumerate(SCHEDULE) if names}
    for j in range(1, NA):
        events.setdefault(NT * j - 2, []).append(functools.partial(next_weights, j))

    def run_events(at):
        for fn in events.get(at, []):
            fn()

    start(w_copies(0, 0))
    start(x_copies(0))
    barrier = pltpu.get_barrier_semaphore()
    for dev in (p.dev_c, p.dev_x, p.dev_y, p.dev_z):
        pl.semaphore_signal(barrier, inc=1, device_id=dev, device_id_type=MESH)
    pl.semaphore_wait(barrier, 4)
    run_events(0)
    wait(w_copies(0, 0))
    wait(x_copies(0))
    for kind in range(2):
        for u in range(PC):
            g_load(kind, u, u).start()
    for t in range(1, NT):
        start(x_copies(t))
    phase1(0, w13_v.at[0], w2_v.at[0], x_v, dy_v, ab_s, dh_s)

    def step(n, carry, last=False):
        j, t = n // NT, n % NT
        ahead = n if last else n + 1
        j1, t1 = ahead // NT, ahead % NT
        slot, slot1 = j % 2, j1 % 2

        if last:
            run_events(n)
        else:
            g_part(n)
            for at in sorted(events):
                if 0 < at < n_steps - 1:
                    pl.when(n == at)(functools.partial(run_events, at))
        when((t == 0) & (j >= 2), lambda: wait(out_copies(j - 2, slot)))
        if not last:
            when((t == NT - 1) & (j + 1 < NA), lambda: wait(w_copies(j + 1, 1 - slot)))
            when(n + 1 < NT, lambda: wait(x_copies(t1)))

        elementwise(ab_s, dh_s, dab_s, h_s)
        if not last:
            phase1(t1, w13_v.at[slot1], w2_v.at[slot1], x_v, dy_v, ab_s, dh_s)
        phase2(t, j > 0, w13_v.at[slot], x_v, dy_v, dab_s, h_s, acc_v, dw13_v.at[slot], dw2_v.at[slot])
        when(t == NT - 1, lambda: start(out_copies(j, slot)))
        when(j == NA - 1, lambda: acc_copy(t).start())
        return carry

    lax.fori_loop(0, n_steps - 1, step, 0)
    step(n_steps - 1, 0, last=True)

    run_events(n_steps)
    if NA < 7:
        arrive(0, 6)
    else:
        by_role(0, True, lambda: arrive(0, 6))
    arrive(1, 0)
    for rid in (4, 5, 6):
        arrive(1, rid)
    for way in range(2):
        z_copy(way).wait()
        s_copy(way).wait()
        r3_copy(way).wait_send()
    for i in range(12):
        pair_copy(i).wait_send()
    for q in range(2):
        for m in range(3):
            ax_copy(q, m).wait_send()
            by_copy(q, m).wait_send()
    for k in range(2):
        for sid in range(5):
            wait_sent(k, sid)

    for k in range(2):
        def relayed(k=k):
            for sid in range(5, 9):
                wait_sent(k, sid)
        pl.when(role[k])(relayed)
    for j in (NA - 2, NA - 1):
        wait(out_copies(j, j % 2))
    for t in range(NT):
        acc_copy(t).wait()


def last_kernel(x_h, dy_h, lw1, lw3, lw2, lv1, lv3, lv2, v1_h, v3_h, v2_h, acc_h, dwa_h, s_h, rz_h,
                dx_h, gn_h, dw_h, o1_h, o3_h, o2_h,
                x_v, dy_v, w13_v, w2_v, acc_v, dw13_v, dw2_v, ab_s, dh_s, dab_s, h_s,
                big, vg_v, vu_v, vd_v, s_v, rz_v, gn_v,
                xs, ws, os, accs, dxs, ins, outs, vin, vout, sz, gs):
    p = Place()
    nb = 8 - NA
    n_steps = nb * NT

    def x_copies(t):
        return (pltpu.make_async_copy(x_h.at[rows_of(t)], x_v.at[rows_of(t)], xs.at[0, t]),
                pltpu.make_async_copy(dy_h.at[rows_of(t)], dy_v.at[rows_of(t)], xs.at[1, t]))

    def acc_copy(t):
        return pltpu.make_async_copy(acc_h.at[rows_of(t)], acc_v.at[rows_of(t)], accs.at[t])

    def dx_copy(t):
        return pltpu.make_async_copy(dy_v.at[rows_of(t)], dx_h.at[rows_of(t)], dxs.at[t])

    def w_copies(j, slot):
        b = p.order(NA + j)
        return weight_copies(tuple(a.at[b] for a in (lw1, lw3, lw2)), w13_v.at[slot], w2_v.at[slot], ws.at[slot])

    def out_copies(j, slot):
        cols = cols_of(p.order(NA + j))
        return (pltpu.make_async_copy(dw13_v.at[slot, :, pl.ds(0, FB)], dw_h.at[0, :, cols], os.at[slot, 0]),
                pltpu.make_async_copy(dw13_v.at[slot, :, pl.ds(FB, FB)], dw_h.at[1, :, cols], os.at[slot, 1]),
                pltpu.make_async_copy(dw2_v.at[slot], dw_h.at[2, :, cols], os.at[slot, 2]))

    moves = [(dwa_h.at[j, m], dw_h.at[m, :, cols_of(p.order(j))]) for j in range(NA) for m in range(3)]

    def dw_copies(g, way):
        half, copies = g % 2, []
        for k, (src, dst) in enumerate(moves[g::DW_GROUPS]):
            if way == 0:
                copies.append(pltpu.make_async_copy(src, big.at[half, k], ins.at[half, k]))
            else:
                copies.append(pltpu.make_async_copy(big.at[half, k], dst, outs.at[half, k]))
        return copies

    def v_loads(m):
        own, got, buf = ((v1_h, lv1, vg_v), (v3_h, lv3, vu_v), (v2_h, lv2, vd_v))[m]
        copies = []
        for j in range(8):
            b = p.order(j)
            dst = buf.at[pl.ds(pl.multiple_of(b * FB, FB), FB)] if m == 2 else buf.at[:, cols_of(b)]
            copies.append(pltpu.make_async_copy(own if j == 0 else got.at[b], dst, vin.at[m, j]))
        return copies

    def v_store(m):
        src, dst = ((vg_v, o1_h), (vu_v, o3_h), (vd_v, o2_h))[m]
        return pltpu.make_async_copy(src, dst, vout.at[m])

    def sz_copies():
        return (pltpu.make_async_copy(s_h, s_v, sz.at[0]), pltpu.make_async_copy(rz_h, rz_v, sz.at[1]))

    def gn_copy():
        return pltpu.make_async_copy(gn_v, gn_h, gs.at[0])

    start(w_copies(0, 0))
    start(x_copies(0))
    wait(w_copies(0, 0))
    wait(x_copies(0))
    start(x_copies(1))
    acc_copy(0).start()
    phase1(0, w13_v.at[0], w2_v.at[0], x_v, dy_v, ab_s, dh_s)

    def dw_next():
        wait(sz_copies())
        for m in range(3):
            gn_v[m] = s_v[m].astype(f32) + rz_v[m].astype(f32)
        gn_copy().start()

    def pass_step(k):
        if 1 <= k <= DW_GROUPS:
            wait(dw_copies(k - 1, 0))
            start(dw_copies(k - 1, 1))
        if k < DW_GROUPS:
            if k >= 2:
                wait(dw_copies(k - 2, 1))
            start(dw_copies(k, 0))
        for m in range(3):
            if k == V_AT[m]:
                start(v_loads(m))
            if k == V_AT[m] + V_LAG:
                wait(v_loads(m))
                v_store(m).start()

    def step(n, carry, last=False):
        j, t = n // NT, n % NT
        ahead = n if last else n + 1
        j1, t1 = ahead // NT, ahead % NT
        slot, slot1 = j % 2, j1 % 2

        def more_loads():
            for i in range(1, nb):
                start(w_copies(i, i))
            start(sz_copies())

        if last:
            pass_step(n)
            when(n < NT, lambda: acc_copy(t).wait())
        else:
            when(n + 1 < NT, lambda: wait(x_copies(t1)))
            when(n + 2 < NT, lambda: start(x_copies(t + 2)))
            when(n + 1 < NT, lambda: acc_copy(t + 1).start())
            when(n < NT, lambda: acc_copy(t).wait())
            when((t == NT - 1) & (j + 1 < nb), lambda: wait(w_copies(j + 1, 1 - slot)))
            when(n == 1, more_loads)
            for k in range(n_steps - 1):
                pl.when(n == k)(functools.partial(pass_step, k))
            when(n == NEXT_AT, dw_next)

        elementwise(ab_s, dh_s, dab_s, h_s)
        if not last:
            phase1(t1, w13_v.at[slot1], w2_v.at[slot1], x_v, dy_v, ab_s, dh_s)
        phase2(t, None, w13_v.at[slot], x_v, dy_v, dab_s, h_s, acc_v, dw13_v.at[slot], dw2_v.at[slot])

        when(t == NT - 1, lambda: start(out_copies(j, slot)))

        def finish():
            dy_v[rows_of(t), :] = acc_v[rows_of(t), :].astype(bf16)
            dx_copy(t).start()
        when(j == nb - 1, finish)
        return carry

    lax.fori_loop(0, n_steps - 1, step, 0)
    step(n_steps - 1, 0, last=True)
    for t in range(NT):
        dx_copy(t).wait()
    for g in (DW_GROUPS - 2, DW_GROUPS - 1):
        wait(dw_copies(g, 1))
    for m in range(3):
        v_store(m).wait()
    for j in range(nb):
        wait(out_copies(j, j))
    gn_copy().wait()


def compute_scratch(slots):
    return [pltpu.VMEM((TOK, D), bf16), pltpu.VMEM((TOK, D), bf16),
            pltpu.VMEM((slots, D, 2 * FB), bf16), pltpu.VMEM((slots, FB, D), bf16),
            pltpu.VMEM((TOK, D), f32), pltpu.VMEM((slots, D, 2 * FB), f32), pltpu.VMEM((slots, D, FB), f32),
            pltpu.VMEM((T, 2 * FB), f32), pltpu.VMEM((T, FB), f32),
            pltpu.VMEM((T, 2 * FB), bf16), pltpu.VMEM((T, FB), bf16)]


def solution(mesh):
    anys = pl.BlockSpec(memory_space=pl.ANY)
    dma = pltpu.SemaphoreType.DMA
    sds = jax.ShapeDtypeStruct

    def device_step(x_loc, dy_loc, w_gate, w_up, w_down, v_gate, v_up, v_down, g_next):
        land = [sds((8, D, FB), bf16), sds((8, D, FB), bf16), sds((8, FB, D), bf16)]
        *gathered, acc, dw_part, g_sum, g_other = pl.pallas_call(
            main_kernel,
            out_shape=land + land + [sds((TOK, D), f32), sds((NA, 3, D, FB), f32),
                                     sds((3, D, FB), bf16), sds((3, D, FB), bf16)],
            in_specs=[anys] * 9, out_specs=[anys] * 10,
            scratch_shapes=compute_scratch(2) + [
                pltpu.VMEM((2, PC, D, FB), f32), pltpu.VMEM((12, D, FB), bf16), pltpu.VMEM((12, D, FB), bf16),
                pltpu.VMEM((2, 3, HALF, FB), bf16), pltpu.VMEM((2, 3, HALF, FB), bf16),
                pltpu.VMEM((2, 3, HALF, FB), bf16),
                dma((2, NT)), dma((2, 3)), dma((2, 3)), dma((NT,)), dma((2, PC)), dma((12,)), dma((12,)),
                dma((2, 3)), dma((2, 3)), dma((2, 3)), dma((2, 3)), dma((2,)), dma((2,)), dma((2,)), dma((2,)),
                dma((2,)), dma((2, 9, 3)), dma((2, 7, 3))],
            compiler_params=pltpu.CompilerParams(
                collective_id=0, has_side_effects=True, vmem_limit_bytes=VMEM_LIMIT),
            name='main_part',
        )(x_loc, dy_loc, w_gate, w_up, w_down, v_gate, v_up, v_down, g_next)
        n_big = -(-3 * NA // DW_GROUPS)
        dx, grad_next, grad_local, vg, vu, vd = pl.pallas_call(
            last_kernel,
            out_shape=[sds((TOK, D), bf16), sds((3, D, FB), f32), sds((3, D, 8 * FB), f32),
                       sds((D, 8 * FB), bf16), sds((D, 8 * FB), bf16), sds((8 * FB, D), bf16)],
            in_specs=[anys] * 15, out_specs=[anys] * 6,
            scratch_shapes=compute_scratch(min(2, 8 - NA)) + [
                pltpu.VMEM((2, n_big, D, FB), f32),
                pltpu.VMEM((D, 8 * FB), bf16), pltpu.VMEM((D, 8 * FB), bf16), pltpu.VMEM((8 * FB, D), bf16),
                pltpu.VMEM((3, D, FB), bf16), pltpu.VMEM((3, D, FB), bf16), pltpu.VMEM((3, D, FB), f32),
                dma((2, NT)), dma((2, 3)), dma((2, 3)), dma((NT,)), dma((NT,)), dma((2, n_big)), dma((2, n_big)), dma((3, 8)), dma((3,)),
                dma((2,)), dma((1,))],
            compiler_params=pltpu.CompilerParams(vmem_limit_bytes=VMEM_LIMIT),
            name='last_part',
        )(x_loc, dy_loc, *gathered, v_gate, v_up, v_down, acc, dw_part, g_sum, g_other)
        return dx, grad_next, grad_local[None], vg, vu, vd

    row_spec = P(ALL_AXES, None)
    col_shard = P(None, FSDP_AXES)
    row_shard = P(FSDP_AXES, None)
    dev_spec = P(ALL_AXES, None, None, None)
    return jax.shard_map(
        device_step, mesh=mesh,
        in_specs=(row_spec, row_spec, col_shard, col_shard, row_shard, col_shard, col_shard, row_shard, dev_spec),
        out_specs=(row_spec, P(None, None, FSDP_AXES), dev_spec, P(), P(), P()),
        check_vma=False)
```
